128 devices in a mesh: dev: 128 (over z, x, y, core).
Axes of the slice: x: 4, y: 4, z: 4, core: 2. Of those that a mesh axis runs over, the one named last changes fastest.
Arguments:
- factors: bfloat16 [1024, 192, 256], P('dev'), may hold values from -6 to 6
- orbital_owner: int32 [1024], replicated, may hold values from 0 to 127, as said below
- tile_orbitals: int32 [1024, 7], P('dev'), may hold values from 0 to 1023, as said below
- projectors: bfloat16 [12288, 192, 128], P('dev'), may hold values from -0.4375 to 0.4375
- amplitudes: float32 [12288, 128, 128], P('dev'), may hold values from -0.3125 to 0.3125
- ranks: int32 [12288], P('dev'), may hold values from 32 to 128, as said below
- pair_energies: float32 [12288, 128], P('dev'), may hold values from 0.5 to 4
- orbital_energies: float32 [1024], replicated, may hold values from 0.25 to 2
Outputs:
- new_amplitudes: float32 [12288, 128, 128], P('dev')
- orbital_sums: bfloat16 [1024, 192, 256], P('dev')
The draws below stay inside these ranges and needn't reach their ends.
Inputs may be any that keep to these rules, and one draw needn't show every extreme that they name: `orbital_owner`: orbitals o and o + 128 have the same owner, and each device owns 8 orbitals. `tile_orbitals`: rows 8 d to 8 d + 7 are the tiles of device d. A row holds 4 consecutive orbital numbers, then 3 consecutive ones; its 12 pairs are rows 12 t + 3 a + b of the pair arrays. The tiles of one device name no orbital twice, and at most 1 orbitals of one owner; some device reaches 1 in every draw. `ranks`: some pair has rank 128.
All inputs are finite; a program needn't handle non-finite values.
Results may differ from the reference program's by a relative error of at most 0.007.
Values may be sent and summed in bfloat16 or wider, within the bound.
No kernel may reach another device: no remote copies, remote signals or barrier semaphores. Data moves between devices by JAX's collectives and lax.ppermute only.
A program may use at most 128 MiB of HBM per device.

```python
import math
import jax
import jax.numpy as jnp
from jax import lax

NAUX = 256
NV = 192
R = 128
ORB_DEV = 8
TILES_DEV = 8
NO = 1024
TILES = 1024
PAIRS_DEV = 96
PAIRS = 12288
N_DEV = 128


def draw_orbital_owner(key, part):
    owner_perm = jax.random.permutation(jax.random.fold_in(key, 11), N_DEV)
    return owner_perm[jnp.arange(NO) % N_DEV].astype(jnp.int32)


def draw_tile_orbitals(key, part):
    positions = N_DEV // 8
    offsets = jax.random.randint(jax.random.fold_in(key, 21), (N_DEV,), 0, positions)
    level_base_i = jax.random.randint(jax.random.fold_in(key, 22), (N_DEV,), 0, ORB_DEV)
    level_base_j = jax.random.randint(jax.random.fold_in(key, 23), (N_DEV,), 0, ORB_DEV)
    tile_local = jnp.arange(TILES_DEV)
    block_pos = (tile_local[None, :] + offsets[:, None]) % positions
    level_shift = tile_local[None, :] // positions
    level_i = (level_base_i[:, None] + level_shift) % ORB_DEV
    level_j = (level_base_j[:, None] + level_shift) % ORB_DEV
    block_start = 8 * block_pos
    orbits_i = block_start[:, :, None] + jnp.arange(4)[None, None, :] + N_DEV * level_i[:, :, None]
    orbits_j = block_start[:, :, None] + 4 + jnp.arange(3)[None, None, :] + N_DEV * level_j[:, :, None]
    return jnp.concatenate([orbits_i, orbits_j], axis=2).reshape(TILES, 7).astype(jnp.int32)


def draw_ranks(key, part):
    rank_low = R // 4
    rank_upper = jax.random.randint(jax.random.fold_in(key, 31), (N_DEV,), rank_low, R + 1)
    raw_bits = jax.random.randint(jax.random.fold_in(key, 32), (PAIRS,), 0, 1 << 20)
    device_of = jnp.arange(PAIRS) // PAIRS_DEV
    ranks_drawn = rank_low + raw_bits % (rank_upper[device_of] - rank_low + 1)
    chosen = jax.random.randint(jax.random.fold_in(key, 33), (), 0, PAIRS)
    return jnp.where(jnp.arange(PAIRS) == chosen, R, ranks_drawn).astype(jnp.int32)


def shard_levels(rng, shape, split, least, high):
    level, own = 1.0, jax.random.fold_in(rng, 6)
    for axis_at, parts in split:
        draws = jnp.exp(jax.random.uniform(jax.random.fold_in(own, axis_at), (parts,), jnp.float32, least / len(split), high / len(split)))
        level = level * jnp.repeat(draws, shape[axis_at] // parts).reshape([-1 if axis == axis_at else 1 for axis in range(len(shape))])
    return level


def centred(rng, shape, spread, limit, shards=(), held_as=jnp.bfloat16):
    factor_of = shard_levels(rng, shape, shards, -0.22, 0.18) if shards else 1.0
    entries = jax.random.normal(rng, shape, jnp.float32) * spread * factor_of
    return jnp.minimum(jnp.maximum(entries, -limit), limit).astype(held_as)


def setup_inputs(seed: int = 0) -> dict:
    streams_of = jax.random.split(jax.random.key(seed), 9)
    factors = centred(streams_of[0], (NO, NV, NAUX), 0.4, 6.0, ((0, 128),))
    orbital_owner = draw_orbital_owner(jax.random.fold_in(streams_of[8], 71), 0)
    tile_orbitals = draw_tile_orbitals(jax.random.fold_in(streams_of[8], 71), 0)
    projectors = centred(streams_of[3], (PAIRS, NV, R), NV ** -0.5, 0.4375, ((0, 128),))
    amplitudes = centred(streams_of[4], (PAIRS, R, R), 0.02, 0.3125, ((0, 128),), jnp.float32)
    ranks = draw_ranks(jax.random.fold_in(streams_of[8], 71), 0)
    pair_energies = jnp.clip(jnp.exp(math.log(4.0) - 2.0794415 * jax.random.uniform(streams_of[6], (PAIRS, R), jnp.float32) ** shard_levels(streams_of[6], (PAIRS, R), ((0, 128),), -0.2, 0.2)), 0.5, 4.0)
    orbital_energies = jnp.clip(jnp.exp(jax.random.uniform(streams_of[7], (NO,), jnp.float32, math.log(0.25), math.log(2.0))), 0.25, 2.0)
    return {"factors": factors, "orbital_owner": orbital_owner, "tile_orbitals": tile_orbitals, "projectors": projectors, "amplitudes": amplitudes, "ranks": ranks, "pair_energies": pair_energies, "orbital_energies": orbital_energies}


def masked_projectors(projectors, ranks):
    rank_keep = (jnp.arange(R)[None, :] < ranks[:, None]).astype(jnp.bfloat16)
    return projectors * rank_keep[:, None, :]


def tile_projections(rows_i, rows_j, tile_masks):
    masks_float = tile_masks.astype(jnp.float32)
    proj_i = jnp.einsum('avn,abvr->abrn', rows_i.astype(jnp.float32), masks_float).astype(jnp.bfloat16)
    proj_j = jnp.einsum('bvn,abvr->abrn', rows_j.astype(jnp.float32), masks_float).astype(jnp.bfloat16)
    return proj_i, proj_j


def reference(factors, orbital_owner, tile_orbitals, projectors, amplitudes, ranks, pair_energies, orbital_energies):
    storage = (orbital_owner[tile_orbitals] * ORB_DEV + tile_orbitals // N_DEV).astype(jnp.int32)
    masked = masked_projectors(projectors, ranks).reshape(TILES, 4, 3, NV, R)
    amp_half = amplitudes.astype(jnp.bfloat16).reshape(TILES, 4, 3, R, R)

    def accumulate(running, tile_items):
        tile_rows, tile_masks, tile_amps = tile_items
        factor_rows = factors[tile_rows]
        proj_i, proj_j = tile_projections(factor_rows[:4], factor_rows[4:], tile_masks)
        amp_float = tile_amps.astype(jnp.float32)
        cycle_i = jnp.einsum('abrc,abcn->abrn', amp_float, proj_j.astype(jnp.float32)).astype(jnp.bfloat16)
        cycle_j = jnp.einsum('abrc,abrn->abcn', amp_float, proj_i.astype(jnp.float32)).astype(jnp.bfloat16)
        masks_float = tile_masks.astype(jnp.float32)
        sum_i = jnp.einsum('abvr,abrn->avn', masks_float, cycle_i.astype(jnp.float32))
        sum_j = jnp.einsum('abvr,abrn->bvn', masks_float, cycle_j.astype(jnp.float32))
        partial_value = jnp.concatenate([sum_i, sum_j], axis=0).astype(jnp.bfloat16)
        partial_value = lax.optimization_barrier(partial_value).astype(jnp.float32)
        return running.at[tile_rows].add(partial_value), None

    totals, _ = lax.scan(accumulate, jnp.zeros((NO, NV, NAUX), jnp.float32), (storage, masked, amp_half))
    orbital_sums = totals.astype(jnp.bfloat16)
    energy = pair_energies.reshape(TILES, 4, 3, R)
    rank_keep = (jnp.arange(R)[None, :] < ranks[:, None]).astype(jnp.float32).reshape(TILES, 4, 3, R)
    occ_gaps = orbital_energies[tile_orbitals]

    def update(tile_items):
        tile_rows, tile_masks, tile_energy, tile_keep, tile_gaps = tile_items
        factor_rows = factors[tile_rows]
        sum_rows = orbital_sums[tile_rows]
        proj_i, proj_j = tile_projections(factor_rows[:4], factor_rows[4:], tile_masks)
        corr_i, corr_j = tile_projections(sum_rows[:4], sum_rows[4:], tile_masks)
        residual = jnp.einsum('abrn,abcn->abrc', proj_i.astype(jnp.float32), proj_j.astype(jnp.float32))
        residual = residual + jnp.einsum('abrn,abcn->abrc', proj_i.astype(jnp.float32), corr_j.astype(jnp.float32))
        residual = residual + jnp.einsum('abrn,abcn->abrc', corr_i.astype(jnp.float32), proj_j.astype(jnp.float32))
        denominator = tile_energy[:, :, :, None] + tile_energy[:, :, None, :]
        denominator = denominator + tile_gaps[:4, None, None, None] + tile_gaps[None, 4:, None, None]
        return -(tile_keep[:, :, :, None] * tile_keep[:, :, None, :]) * residual / denominator

    updated = lax.map(update, (storage, masked, energy, rank_keep, occ_gaps))
    return updated.reshape(PAIRS, R, R), orbital_sums
```

```python
import functools

import jax
import jax.numpy as jnp
from jax import lax
from jax.experimental import pallas as pl
from jax.experimental.pallas import tpu as pltpu
from jax.sharding import Mesh
from jax.sharding import PartitionSpec as P

DEV = ("dev_0", "dev_1", "dev_2", "dev_3")
CORE = "dev_3"
RING = 4
ORDERS = ((0, 1, 2), (1, 2, 0), (2, 0, 1))
STRIDES = (32, 8, 2)


BF16 = jnp.bfloat16
F32 = jnp.float32
ANY = pl.BlockSpec(memory_space=pl.ANY)
SMEM = pl.BlockSpec(memory_space=pltpu.SMEM)


def shift(value, axis, step, flip=0):
    if step % RING == 0 and flip == 0:
        return value
    pairs = []
    for place in range(RING):
        for core in range(2):
            pairs.append((place * 2 + core, ((place + step) % RING) * 2 + (core ^ flip)))
    return lax.ppermute(value, (DEV[axis], CORE), pairs)


def dot(a, b, dims):
    return lax.dot_general(a, b, (dims, ((), ())), preferred_element_type=F32)


def owner_of(coords, order, q1, q2):
    d1, d2, d3 = order
    pos1 = (coords[d1] + RING - q1) % RING
    pos2 = (coords[d2] + RING - q2) % RING
    return pos1 * STRIDES[d1] + pos2 * STRIDES[d2] + coords[d3] * STRIDES[d3] + coords[3]


def pack_kernel(order, coords, table, g0, g1, g2, g3, *refs):
    outs, buf, sem_in, sem_out = refs[:8], refs[8], refs[9], refs[10]
    gathered = (g0, g1, g2, g3)
    for kf in range(8):
        for q2 in range(RING):
            for q1 in range(RING):
                level = jnp.clip(table[kf, owner_of(coords, order, q1, q2)], 0, 7)
                pltpu.make_async_copy(
                    gathered[q2].at[q1 * 8 + level], buf.at[kf, q2 * RING + q1], sem_in.at[kf]
                ).start()
    for kf in range(8):
        pltpu.make_async_copy(buf.at[kf], buf.at[kf], sem_in.at[kf]).wait()
        pltpu.make_async_copy(buf.at[kf], outs[kf], sem_out.at[kf]).start()
    for kf in range(8):
        pltpu.make_async_copy(buf.at[kf], outs[kf], sem_out.at[kf]).wait()


def pack(order, coords, table, gathered, rows, width):
    slot = jax.ShapeDtypeStruct((16, rows, width), BF16)
    return pl.pallas_call(
        functools.partial(pack_kernel, order),
        in_specs=[SMEM, SMEM] + [ANY] * 4,
        out_specs=[ANY] * 8,
        out_shape=[slot] * 8,
        scratch_shapes=[
            pltpu.VMEM((8, 16, rows, width), BF16),
            pltpu.SemaphoreType.DMA((8,)),
            pltpu.SemaphoreType.DMA((8,)),
        ],
        name="pack",
    )(coords, table, *gathered)


def combine_kernel(order, coords, table, *refs):
    slots, outs, acc = refs[:8], refs[8:9], refs[9]
    q2 = pl.program_id(0)
    for q1 in range(RING):
        acc[...] = jnp.zeros_like(acc)
        for kf in range(8):
            level = table[kf, owner_of(coords, order, q1, q2)]

            @pl.when(level >= 0)
            def _():
                place = jnp.clip(level, 0, 7)
                acc[place] = acc[place] + slots[kf][q1].astype(F32)

        outs[0][0, q1] = acc[...].astype(BF16)


def combine(order, coords, table, slots, rows, width):
    block = pl.BlockSpec((RING, rows, width), lambda q: (q, 0, 0))
    return pl.pallas_call(
        functools.partial(combine_kernel, order),
        grid=(RING,),
        in_specs=[SMEM, SMEM] + [block] * 8,
        out_specs=[pl.BlockSpec((1, RING, 8, rows, width), lambda q: (q, 0, 0, 0, 0))],
        out_shape=[jax.ShapeDtypeStruct((RING, RING, 8, rows, width), BF16)],
        scratch_shapes=[pltpu.VMEM((8, rows, width), F32)],
        name="combine",
    )(coords, table, *slots)[0]


def fetch_items(arrays, which, slot, items, sem, tile, rows, buf):
    for entry in range(7):
        for part in range(3):
            at = slot[part * 56 + tile * 7 + entry]
            index = which[part * 56 + tile * 7 + entry]
            for kf in range(8):

                @pl.when(index == kf)
                def _():
                    pltpu.make_async_copy(
                        arrays[part * 8 + kf].at[at],
                        items.at[buf, entry, pl.ds(part * rows, rows)],
                        sem.at[buf],
                    ).start()


def wait_items(items, sem, buf):
    pltpu.make_async_copy(items.at[buf], items.at[buf], sem.at[buf]).wait()


def masked_pair(projectors, ranks, tile, pair):
    keep = lax.broadcasted_iota(jnp.int32, projectors.shape[1:], 1) < ranks[tile * 12 + pair]
    return jnp.where(keep, projectors[pair], jnp.zeros_like(projectors[pair]))


def cycle_kernel(rows, which, slot, ranks, *refs):
    arrays = refs[:24]
    projectors, amplitudes = refs[24:26]
    outs = refs[26:50]
    proj_i_out, proj_j_out = refs[50:52]
    items, partial, sums_j, sem_in, sem_out = refs[52:]
    tile = pl.program_id(0)
    tiles = pl.num_programs(0)
    buf = lax.rem(tile, 2)

    @pl.when(tile == 0)
    def _():
        fetch_items(arrays, which, slot, items, sem_in, 0, rows, 0)

    @pl.when(tile + 1 < tiles)
    def _():
        fetch_items(arrays, which, slot, items, sem_in, tile + 1, rows, 1 - buf)

    @pl.when(tile >= 2)
    def _():
        wait_items(partial, sem_out, buf)

    wait_items(items, sem_in, buf)
    for a in range(4):
        sum_i = None
        for b in range(3):
            pair = 3 * a + b
            masked = masked_pair(projectors, ranks, tile, pair)
            proj_i = dot(masked, items[buf, a], ((0,), (0,))).astype(BF16)
            proj_j = dot(masked, items[buf, 4 + b], ((0,), (0,))).astype(BF16)
            proj_i_out[pair] = proj_i
            proj_j_out[pair] = proj_j
            amp = amplitudes[pair].astype(BF16)
            cycle_i = dot(amp, proj_j, ((1,), (0,))).astype(BF16)
            cycle_j = dot(amp, proj_i, ((0,), (0,))).astype(BF16)
            add_i = dot(masked, cycle_i, ((1,), (0,)))
            add_j = dot(masked, cycle_j, ((1,), (0,)))
            sum_i = add_i if b == 0 else sum_i + add_i
            if a == 0:
                sums_j[b] = add_j
            elif a < 3:
                sums_j[b] = sums_j[b] + add_j
            else:
                partial[buf, 4 + b] = (sums_j[b] + add_j).astype(BF16)
        partial[buf, a] = sum_i.astype(BF16)
    for entry in range(7):
        for part in range(3):
            at = slot[part * 56 + tile * 7 + entry]
            index = which[part * 56 + tile * 7 + entry]
            for kf in range(8):

                @pl.when(index == kf)
                def _():
                    pltpu.make_async_copy(
                        partial.at[buf, entry, pl.ds(part * rows, rows)],
                        outs[part * 8 + kf].at[at],
                        sem_out.at[buf],
                    ).start()

    @pl.when(tile == tiles - 1)
    def _():
        wait_items(partial, sem_out, buf)

        @pl.when(tiles >= 2)
        def _():
            wait_items(partial, sem_out, 1 - buf)


def cycle(which, slot, ranks, arrays, projectors, amplitudes, tiles, rows, width):
    pairs, virt, rank = projectors.shape
    slots = jax.ShapeDtypeStruct((16, rows, width), BF16)
    proj = jax.ShapeDtypeStruct((pairs, rank, width), BF16)
    block = lambda *shape: pl.BlockSpec((12,) + shape, lambda t: (t, 0, 0))
    return pl.pallas_call(
        functools.partial(cycle_kernel, rows),
        grid=(tiles,),
        in_specs=[SMEM] * 3 + [ANY] * 24 + [block(virt, rank), block(rank, rank)],
        out_specs=[ANY] * 24 + [block(rank, width)] * 2,
        out_shape=[slots] * 24 + [proj] * 2,
        scratch_shapes=[
            pltpu.VMEM((2, 7, virt, width), BF16),
            pltpu.VMEM((2, 7, virt, width), BF16),
            pltpu.VMEM((3, virt, width), F32),
            pltpu.SemaphoreType.DMA((2,)),
            pltpu.SemaphoreType.DMA((2,)),
        ],
        compiler_params=pltpu.CompilerParams(vmem_limit_bytes=48 * 1024 * 1024),
        name="cycle",
    )(which, slot, ranks, *arrays, projectors, amplitudes)


def update_kernel(rows, which, slot, ranks, gaps, *refs):
    arrays = refs[:24]
    projectors, proj_i_in, proj_j_in, energies, out, items, sem_in = refs[24:]
    tile = pl.program_id(0)
    tiles = pl.num_programs(0)
    buf = lax.rem(tile, 2)

    @pl.when(tile == 0)
    def _():
        fetch_items(arrays, which, slot, items, sem_in, 0, rows, 0)

    @pl.when(tile + 1 < tiles)
    def _():
        fetch_items(arrays, which, slot, items, sem_in, tile + 1, rows, 1 - buf)

    wait_items(items, sem_in, buf)
    for a in range(4):
        for b in range(3):
            pair = 3 * a + b
            masked = masked_pair(projectors, ranks, tile, pair)
            corr_i = dot(masked, items[buf, a], ((0,), (0,))).astype(BF16)
            corr_j = dot(masked, items[buf, 4 + b], ((0,), (0,))).astype(BF16)
            proj_i = proj_i_in[pair]
            proj_j = proj_j_in[pair]
            residual = dot(proj_i, proj_j, ((1,), (1,)))
            residual = residual + dot(proj_i, corr_j, ((1,), (1,)))
            residual = residual + dot(corr_i, proj_j, ((1,), (1,)))
            along = jnp.broadcast_to(energies[0, pl.ds(pair, 1)], residual.shape)
            gap = gaps[tile * 7 + a] + gaps[tile * 7 + 4 + b]
            bottom = along + along.T + gap
            limit = ranks[tile * 12 + pair]
            row = lax.broadcasted_iota(jnp.int32, residual.shape, 0)
            col = lax.broadcasted_iota(jnp.int32, residual.shape, 1)
            keep = (row < limit) & (col < limit)
            out[pair] = jnp.where(keep, -residual / bottom, 0.0)


def update(which, slot, ranks, gaps, arrays, projectors, proj_i, proj_j, energies, tiles, rows, width):
    pairs, virt, rank = projectors.shape
    block = lambda *shape: pl.BlockSpec((12,) + shape, lambda t: (t, 0, 0))
    return pl.pallas_call(
        functools.partial(update_kernel, rows),
        grid=(tiles,),
        in_specs=[SMEM] * 4
        + [ANY] * 24
        + [block(virt, rank), block(rank, width), block(rank, width)]
        + [pl.BlockSpec((1, 12, rank), lambda t: (t, 0, 0))],
        out_specs=block(rank, rank),
        out_shape=jax.ShapeDtypeStruct((pairs, rank, rank), F32),
        scratch_shapes=[
            pltpu.VMEM((2, 7, virt, width), BF16),
            pltpu.SemaphoreType.DMA((2,)),
        ],
        compiler_params=pltpu.CompilerParams(vmem_limit_bytes=48 * 1024 * 1024),
        name="update",
    )(which, slot, ranks, gaps, *arrays, projectors, proj_i, proj_j, energies.reshape(tiles, 12, rank))


def deliver(order, coords, table, gathered, rows, width):
    packed = pack(order, coords, table, gathered, rows, width)
    return [shift(packed[k * 2 + f], order[2], k, f) for k in range(RING) for f in range(2)]


def body(
    factors,
    orbital_owner,
    tile_orbitals,
    projectors,
    amplitudes,
    ranks,
    pair_energies,
    orbital_energies,
):
    dev_count = lax.axis_size(DEV)
    tiles = tile_orbitals.shape[0]
    levels, virt, width = factors.shape
    rows = virt // 3
    coords = jnp.stack([lax.axis_index(name) for name in DEV]).astype(jnp.int32)
    my_orbitals = tile_orbitals.reshape(-1)
    owners = orbital_owner[my_orbitals]
    level_of = my_orbitals // dev_count
    hit = owners[:, None] == jnp.arange(dev_count)[None, :]
    want = jnp.sum(jnp.where(hit, level_of[:, None] + 1, 0), axis=0) - 1

    place = [(owners // stride) % RING for stride in STRIDES]
    flips = (owners % 2) ^ coords[3]
    which, slot = [], []
    for d1, d2, d3 in ORDERS:
        away = [(coords[d] - place[d]) % RING for d in range(3)]
        which.append(away[d3] * 2 + flips)
        slot.append(away[d2] * RING + away[d1])
    which = jnp.concatenate(which).astype(jnp.int32)
    slot = jnp.concatenate(slot).astype(jnp.int32)

    want_rows = jnp.pad(want.astype(BF16)[None, :], ((0, 15), (0, width - dev_count)))
    first, lines = [], [None] * 3
    for part, order in enumerate(ORDERS):
        own = factors[:, part * rows : (part + 1) * rows].reshape(levels * rows, width)
        own = jnp.concatenate([own, want_rows], axis=0)
        got = [own] + [shift(own, order[0], k) for k in range(1, RING)]
        first.append([g[: levels * rows].reshape(levels, rows, width) for g in got])
        lines[order[0]] = jnp.stack([g[levels * rows, :dev_count] for g in got])
    second = []
    for part, order in enumerate(ORDERS):
        mine = jnp.concatenate(first[part], axis=0)
        second.append([mine] + [shift(mine, order[1], k) for k in range(1, RING)])
    mine = jnp.stack(lines)
    other = shift(mine, 0, 0, 1)
    tables = []
    for part, order in enumerate(ORDERS):
        both = jnp.stack([mine[order[2]], other[order[2]]], axis=1)
        both = jnp.concatenate([both[:1], both[:0:-1]], axis=0)
        tables.append(both.reshape(2 * RING, dev_count).astype(jnp.int32))
    arrays = []
    for part, order in enumerate(ORDERS):
        arrays += deliver(order, coords, tables[part], second[part], rows, width)

    done = cycle(which, slot, ranks, arrays, projectors, amplitudes, tiles, rows, width)
    proj_i, proj_j = done[24:]

    sums = []
    for part, order in enumerate(ORDERS):
        back = done[part * 8 : part * 8 + 8]
        back = [shift(back[k * 2 + f], order[2], -k, f) for k in range(RING) for f in range(2)]
        held = combine(order, coords, tables[part], back, rows, width)
        got = [shift(held[k], order[1], -k) for k in range(RING)]
        line = []
        for q1 in range(RING):
            total = got[0][q1].astype(F32)
            for k in range(1, RING):
                total = total + got[k][q1].astype(F32)
            line.append(total.astype(BF16))
        got = [shift(line[k], order[0], -k) for k in range(RING)]
        total = got[0].astype(F32)
        for k in range(1, RING):
            total = total + got[k].astype(F32)
        sums.append(total.astype(BF16))
    orbital_sums = jnp.concatenate(sums, axis=1)

    arrays = []
    gathered = []
    for part, order in enumerate(ORDERS):
        mine = jnp.concatenate([shift(sums[part], order[0], k) for k in range(RING)], axis=0)
        gathered.append([shift(mine, order[1], k) for k in range(RING)])
    for part, order in enumerate(ORDERS):
        arrays += deliver(order, coords, tables[part], gathered[part], rows, width)
    gaps = orbital_energies[my_orbitals]
    updated = update(
        which, slot, ranks, gaps, arrays, projectors, proj_i, proj_j, pair_energies, tiles, rows, width
    )
    return updated, orbital_sums


def solution(mesh):
    split = Mesh(mesh.devices.reshape(4, 4, 4, 2), DEV)
    in_specs = (
        P(DEV, None, None),
        P(),
        P(DEV, None),
        P(DEV, None, None),
        P(DEV, None, None),
        P(DEV),
        P(DEV, None),
        P(),
    )
    out_specs = (P(DEV, None, None), P(DEV, None, None))
    return jax.shard_map(body, mesh=split, in_specs=in_specs, out_specs=out_specs, check_vma=False)
```

```python
import functools

import jax
import jax.numpy as jnp
from jax import lax
from jax.experimental import pallas as pl
from jax.experimental.pallas import tpu as pltpu
from jax.sharding import Mesh
from jax.sharding import PartitionSpec as P

DEV = ("dev_0", "dev_1", "dev_2", "dev_3")
CORE = "dev_3"
RING = 4
ORDERS = ((0, 1, 2), (1, 2, 0), (2, 0, 1))
STRIDES = (32, 8, 2)


BF16 = jnp.bfloat16
F32 = jnp.float32
ANY = pl.BlockSpec(memory_space=pl.ANY)
SMEM = pl.BlockSpec(memory_space=pltpu.SMEM)


def shift(value, axis, step, flip=0):
    if step % RING == 0 and flip == 0:
        return value
    pairs = []
    for place in range(RING):
        for core in range(2):
            pairs.append((place * 2 + core, ((place + step) % RING) * 2 + (core ^ flip)))
    return lax.ppermute(value, (DEV[axis], CORE), pairs)


def dot(a, b, dims):
    return lax.dot_general(a, b, (dims, ((), ())), preferred_element_type=F32)


def owner_of(coords, order, q1, q2):
    d1, d2, d3 = order
    pos1 = (coords[d1] + RING - q1) % RING
    pos2 = (coords[d2] + RING - q2) % RING
    return pos1 * STRIDES[d1] + pos2 * STRIDES[d2] + coords[d3] * STRIDES[d3] + coords[3]


DELIVERED = ((1, 0), (3, 0), (2, 0), (1, 1), (3, 1), (2, 1), (0, 1), (0, 0))


def pack_kernel(coords, tables, *refs):
    gathered, outs = refs[:24], refs[24:48]
    buf, sem_in, sem_out = refs[48:]
    sources = []
    for order in ORDERS:
        sources.append([owner_of(coords, order, q1, q2) for q2 in range(RING) for q1 in range(RING)])
    for k, f in DELIVERED:
        kf = k * 2 + f
        for part in range(3):
            for q2 in range(RING):
                for q1 in range(RING):
                    place = q2 * RING + q1
                    level = jnp.clip(tables[part * 8 + kf, sources[part][place]], 0, 7)
                    pltpu.make_async_copy(
                        gathered[part * 8 + q2 * 2 + q1 // 2].at[(q1 % 2) * 8 + level],
                        buf.at[part * 8 + kf, place],
                        sem_in.at[part * 8 + kf],
                    ).start()
    for k, f in DELIVERED:
        for part in range(3):
            at = part * 8 + k * 2 + f
            pltpu.make_async_copy(buf.at[at], buf.at[at], sem_in.at[at]).wait()
            pltpu.make_async_copy(buf.at[at], outs[at], sem_out.at[at]).start()
    for at in range(24):
        pltpu.make_async_copy(buf.at[at], outs[at], sem_out.at[at]).wait()


def pack(coords, tables, gathered, rows, width):
    slot = jax.ShapeDtypeStruct((16, rows, width), BF16)
    return pl.pallas_call(
        pack_kernel,
        in_specs=[SMEM, SMEM] + [ANY] * 24,
        out_specs=[ANY] * 24,
        out_shape=[slot] * 24,
        scratch_shapes=[
            pltpu.VMEM((24, 16, rows, width), BF16),
            pltpu.SemaphoreType.DMA((24,)),
            pltpu.SemaphoreType.DMA((24,)),
        ],
        compiler_params=pltpu.CompilerParams(vmem_limit_bytes=32 * 1024 * 1024),
        name="pack",
    )(coords, tables, *gathered)


HALVES = ((2, 0), (2, 1), (1, 1), (3, 0), (1, 0), (3, 1), (0, 0), (0, 1))


def combine_kernel(order, coords, table, *refs):
    slots, outs = refs[:8], refs[8:16]
    acc, buf, sem = refs[16:]
    step = pl.program_id(0)
    slot_of = lax.rem(step, 2)
    q2 = jnp.int32(HALVES[0][0])
    half = jnp.int32(HALVES[0][1])
    for at, (a, b) in enumerate(HALVES):
        q2 = jnp.where(step == at, a, q2)
        half = jnp.where(step == at, b, half)

    def drain(slot):
        pltpu.make_async_copy(buf.at[slot], outs[0], sem.at[slot]).wait()

    @pl.when(step >= 2)
    def _():
        drain(slot_of)

    for q in range(2):
        source = owner_of(coords, order, half * 2 + q, q2)
        acc[...] = jnp.zeros_like(acc)
        for kf in range(8):
            level = table[kf, source]

            @pl.when(level >= 0)
            def _():
                place = jnp.clip(level, 0, 7)
                acc[place] = acc[place] + slots[kf][q].astype(F32)

        buf[slot_of, q] = acc[...].astype(BF16)
    for at in range(8):

        @pl.when(step == at)
        def _():
            pltpu.make_async_copy(buf.at[slot_of], outs[at], sem.at[slot_of]).start()

    @pl.when(step == 7)
    def _():
        drain(slot_of)
        drain(1 - slot_of)


def half_block(step):
    block = jnp.int32(HALVES[0][0] * 2 + HALVES[0][1])
    for at, (a, b) in enumerate(HALVES):
        block = jnp.where(step == at, a * 2 + b, block)
    return block


def combine(order, coords, table, slots, rows, width):
    block = pl.BlockSpec((2, rows, width), lambda q: (half_block(q), 0, 0))
    outs = pl.pallas_call(
        functools.partial(combine_kernel, order),
        grid=(8,),
        in_specs=[SMEM, SMEM] + [block] * 8,
        out_specs=[ANY] * 8,
        out_shape=[jax.ShapeDtypeStruct((2, 8, rows, width), BF16)] * 8,
        scratch_shapes=[
            pltpu.VMEM((8, rows, width), F32),
            pltpu.VMEM((2, 2, 8, rows, width), BF16),
            pltpu.SemaphoreType.DMA((2,)),
        ],
        name="combine",
    )(coords, table, *slots)
    return dict(zip(HALVES, outs))


def load_slots(arrays, held, sem):
    for part in range(3):
        for kf in range(8):
            pltpu.make_async_copy(
                arrays[part * 8 + kf], held.at[part, pl.ds(kf * 16, 16)], sem.at[part]
            ).start()
    for part in range(3):
        pltpu.make_async_copy(held.at[part], held.at[part], sem.at[part]).wait()


def item(held, where, entry):
    return jnp.concatenate([held[part, where[part * 56 + entry]] for part in range(3)], axis=0)


def mask_pairs(projectors, ranks, tile, turned, masked=None):
    for pair in range(12):
        value = projectors[pair]
        keep = lax.broadcasted_iota(jnp.int32, value.shape, 1) < ranks[tile * 12 + pair]
        value = jnp.where(keep, value, jnp.zeros_like(value))
        if masked is not None:
            masked[pair] = value
        turned[pair] = value.T


def project(turned, held, where, tile, out_i, out_j):
    rank = turned.shape[1]
    for a in range(4):
        stack = jnp.concatenate([turned[3 * a + b] for b in range(3)], axis=0)
        value = dot(stack, item(held, where, tile * 7 + a), ((1,), (0,))).astype(BF16)
        for b in range(3):
            out_i[3 * a + b] = value[b * rank : (b + 1) * rank]
    for b in range(3):
        stack = jnp.concatenate([turned[3 * a + b] for a in range(4)], axis=0)
        value = dot(stack, item(held, where, tile * 7 + 4 + b), ((1,), (0,))).astype(BF16)
        for a in range(4):
            out_j[3 * a + b] = value[a * rank : (a + 1) * rank]


def cycle_kernel(rows, where, ranks, *refs):
    arrays = refs[:24]
    projectors, amplitudes = refs[24:26]
    outs = refs[26:50]
    proj_i, proj_j = refs[50:52]
    held, partial, masked, turned, cycles_i, cycles_j, sem_in, sem_out = refs[52:]
    tile = pl.program_id(0)

    @pl.when(tile == 0)
    def _():
        load_slots(arrays, held, sem_in)

    mask_pairs(projectors, ranks, tile, turned, masked)
    project(turned, held, where, tile, proj_i, proj_j)
    for a in range(4):
        for b in range(3):
            pair = 3 * a + b
            amp = amplitudes[pair].astype(BF16)
            cycles_i[pair] = dot(amp, proj_j[pair], ((1,), (0,))).astype(BF16)
            cycles_j[pair] = dot(amp, proj_i[pair], ((0,), (0,))).astype(BF16)

    def put(entry, value):
        for part in range(3):
            partial[part, where[part * 56 + tile * 7 + entry]] = value[part * rows : (part + 1) * rows]

    for a in range(4):
        pairs = [3 * a + b for b in range(3)]
        left = jnp.concatenate([masked[pair] for pair in pairs], axis=1)
        right = jnp.concatenate([cycles_i[pair] for pair in pairs], axis=0)
        put(a, dot(left, right, ((1,), (0,))).astype(BF16))
    for b in range(3):
        pairs = [3 * a + b for a in range(4)]
        left = jnp.concatenate([masked[pair] for pair in pairs], axis=1)
        right = jnp.concatenate([cycles_j[pair] for pair in pairs], axis=0)
        put(4 + b, dot(left, right, ((1,), (0,))).astype(BF16))

    @pl.when(tile == pl.num_programs(0) - 1)
    def _():
        for k, f in DELIVERED:
            for part in range(3):
                kf = k * 2 + f
                pltpu.make_async_copy(
                    partial.at[part, pl.ds(kf * 16, 16)], outs[part * 8 + kf], sem_out.at[part * 8 + kf]
                ).start()
        for part in range(3):
            for kf in range(8):
                pltpu.make_async_copy(
                    partial.at[part, pl.ds(kf * 16, 16)], outs[part * 8 + kf], sem_out.at[part * 8 + kf]
                ).wait()


def cycle(where, ranks, arrays, projectors, amplitudes, tiles, rows, width):
    pairs, virt, rank = projectors.shape
    slots = jax.ShapeDtypeStruct((16, rows, width), BF16)
    proj = jax.ShapeDtypeStruct((pairs, rank, width), BF16)
    block = lambda *shape: pl.BlockSpec((12,) + shape, lambda t: (t, 0, 0))
    return pl.pallas_call(
        functools.partial(cycle_kernel, rows),
        grid=(tiles,),
        in_specs=[SMEM] * 2 + [ANY] * 24 + [block(virt, rank), block(rank, rank)],
        out_specs=[ANY] * 24 + [block(rank, width)] * 2,
        out_shape=[slots] * 24 + [proj] * 2,
        scratch_shapes=[
            pltpu.VMEM((3, 128, rows, width), BF16),
            pltpu.VMEM((3, 128, rows, width), BF16),
            pltpu.VMEM((12, virt, rank), BF16),
            pltpu.VMEM((12, rank, virt), BF16),
            pltpu.VMEM((12, rank, width), BF16),
            pltpu.VMEM((12, rank, width), BF16),
            pltpu.SemaphoreType.DMA((3,)),
            pltpu.SemaphoreType.DMA((24,)),
        ],
        compiler_params=pltpu.CompilerParams(vmem_limit_bytes=48 * 1024 * 1024),
        name="cycle",
    )(where, ranks, *arrays, projectors, amplitudes)


def update_kernel(where, ranks, gaps, *refs):
    arrays = refs[:24]
    projectors, proj_i_in, proj_j_in, energies, out = refs[24:29]
    held, turned, corr_i, corr_j, sem_in = refs[29:]
    tile = pl.program_id(0)

    @pl.when(tile == 0)
    def _():
        load_slots(arrays, held, sem_in)

    mask_pairs(projectors, ranks, tile, turned)
    project(turned, held, where, tile, corr_i, corr_j)
    rank = turned.shape[1]
    for a in range(4):
        for b in range(3):
            pair = 3 * a + b
            proj_i = proj_i_in[pair]
            proj_j = proj_j_in[pair]
            both = dot(jnp.concatenate([proj_i, corr_i[pair]], axis=0), proj_j, ((1,), (1,)))
            residual = both[:rank] + dot(proj_i, corr_j[pair], ((1,), (1,))) + both[rank:]
            along = jnp.broadcast_to(energies[0, pl.ds(pair, 1)], residual.shape)
            gap = gaps[tile * 7 + a] + gaps[tile * 7 + 4 + b]
            bottom = along + along.T + gap
            limit = ranks[tile * 12 + pair]
            row = lax.broadcasted_iota(jnp.int32, residual.shape, 0)
            col = lax.broadcasted_iota(jnp.int32, residual.shape, 1)
            keep = (row < limit) & (col < limit)
            out[pair] = jnp.where(keep, -residual / bottom, 0.0)


def update(where, ranks, gaps, arrays, projectors, proj_i, proj_j, energies, tiles, rows, width):
    pairs, virt, rank = projectors.shape
    block = lambda *shape: pl.BlockSpec((12,) + shape, lambda t: (t, 0, 0))
    return pl.pallas_call(
        update_kernel,
        grid=(tiles,),
        in_specs=[SMEM] * 3
        + [ANY] * 24
        + [block(virt, rank), block(rank, width), block(rank, width)]
        + [pl.BlockSpec((1, 12, rank), lambda t: (t, 0, 0))],
        out_specs=block(rank, rank),
        out_shape=jax.ShapeDtypeStruct((pairs, rank, rank), F32),
        scratch_shapes=[
            pltpu.VMEM((3, 128, rows, width), BF16),
            pltpu.VMEM((12, rank, virt), BF16),
            pltpu.VMEM((12, rank, width), BF16),
            pltpu.VMEM((12, rank, width), BF16),
            pltpu.SemaphoreType.DMA((3,)),
        ],
        compiler_params=pltpu.CompilerParams(vmem_limit_bytes=48 * 1024 * 1024),
        name="update",
    )(where, ranks, gaps, *arrays, projectors, proj_i, proj_j, energies.reshape(tiles, 12, rank))


def gather_second(lines):
    halves = []
    for line in lines:
        halves.append([jnp.concatenate(line[:2], axis=0), jnp.concatenate(line[2:], axis=0)])
    second = [{(0, 0): lo, (0, 1): hi} for lo, hi in halves]
    for part, order in enumerate(ORDERS):
        second[part][1, 0] = shift(halves[part][0], order[1], 1)
        second[part][3, 1] = shift(halves[part][1], order[1], 3)
    for part, order in enumerate(ORDERS):
        second[part][3, 0] = shift(halves[part][0], order[1], 3)
        second[part][1, 1] = shift(halves[part][1], order[1], 1)
    for part, order in enumerate(ORDERS):
        second[part][2, 0] = shift(second[part][1, 0], order[1], 1)
        second[part][2, 1] = shift(second[part][3, 1], order[1], 3)
    return second


def deliver(coords, tables, second, rows, width):
    gathered = []
    for part in range(3):
        for q2 in range(RING):
            gathered += [second[part][q2, half].reshape(16, rows, width) for half in range(2)]
    packed = pack(coords, jnp.concatenate(tables, axis=0), gathered, rows, width)
    arrays = [None] * 24
    for k, f in DELIVERED:
        for part, order in enumerate(ORDERS):
            at = part * 8 + k * 2 + f
            arrays[at] = shift(packed[at], order[2], k, f)
    return arrays


def add(*terms):
    total = terms[0].astype(F32)
    for term in terms[1:]:
        total = total + term.astype(F32)
    return total.astype(BF16)


def scatter_second(held, order):
    axis = order[1]
    far_lo = shift(held[2, 0], axis, 3)
    far_hi = shift(held[2, 1], axis, 1)
    near_hi = shift(held[1, 1], axis, 3)
    near_lo = shift(held[3, 0], axis, 1)
    via_lo = shift(add(held[1, 0], far_lo), axis, 3)
    via_hi = shift(add(held[3, 1], far_hi), axis, 1)
    line = []
    for q in range(2):
        line.append(add(held[0, 0][q], near_lo[q], via_lo[q]))
    for q in range(2):
        line.append(add(held[0, 1][q], near_hi[q], via_hi[q]))
    return line


def body(
    factors,
    orbital_owner,
    tile_orbitals,
    projectors,
    amplitudes,
    ranks,
    pair_energies,
    orbital_energies,
):
    dev_count = lax.axis_size(DEV)
    tiles = tile_orbitals.shape[0]
    levels, virt, width = factors.shape
    rows = virt // 3
    coords = jnp.stack([lax.axis_index(name) for name in DEV]).astype(jnp.int32)
    my_orbitals = tile_orbitals.reshape(-1)
    owners = orbital_owner[my_orbitals]
    level_of = my_orbitals // dev_count
    hit = owners[:, None] == jnp.arange(dev_count)[None, :]
    want = jnp.sum(jnp.where(hit, level_of[:, None] + 1, 0), axis=0) - 1

    place = [(owners // stride) % RING for stride in STRIDES]
    flips = (owners % 2) ^ coords[3]
    where = []
    for d1, d2, d3 in ORDERS:
        away = [(coords[d] - place[d]) % RING for d in range(3)]
        where.append((away[d3] * 2 + flips) * 16 + away[d2] * RING + away[d1])
    where = jnp.concatenate(where).astype(jnp.int32)

    want_rows = jnp.pad(want.astype(BF16)[None, :], ((0, 15), (0, width - dev_count)))
    size = levels * rows
    first, lines = [], [None] * 3
    for part, order in enumerate(ORDERS):
        own = factors[:, part * rows : (part + 1) * rows].reshape(size, width)
        own = jnp.concatenate([own, want_rows], axis=0)
        got = [shift(own, order[0], k) for k in range(RING)]
        first.append([g[:size] for g in got])
        lines[order[0]] = jnp.stack([g[size, :dev_count] for g in got])
    second = gather_second(first)
    mine = jnp.stack(lines)
    other = shift(mine, 0, 0, 1)
    tables = []
    for part, order in enumerate(ORDERS):
        both = jnp.stack([mine[order[2]], other[order[2]]], axis=1)
        both = jnp.concatenate([both[:1], both[:0:-1]], axis=0)
        tables.append(both.reshape(2 * RING, dev_count).astype(jnp.int32))
    arrays = deliver(coords, tables, second, rows, width)

    done = cycle(where, ranks, arrays, projectors, amplitudes, tiles, rows, width)
    proj_i, proj_j = done[24:]

    back = [None] * 24
    for k, f in DELIVERED:
        for part, order in enumerate(ORDERS):
            at = part * 8 + k * 2 + f
            back[at] = shift(done[at], order[2], -k, f)
    sums, first = [], []
    for part, order in enumerate(ORDERS):
        held = combine(order, coords, tables[part], back[part * 8 : part * 8 + 8], rows, width)
        line = scatter_second(held, order)
        sums.append(add(*[shift(line[k], order[0], -k) for k in range(RING)]))
    orbital_sums = jnp.concatenate(sums, axis=1)
    for part, order in enumerate(ORDERS):
        first.append([shift(sums[part], order[0], k) for k in range(RING)])
    arrays = deliver(coords, tables, gather_second(first), rows, width)
    gaps = orbital_energies[my_orbitals]
    updated = update(
        where, ranks, gaps, arrays, projectors, proj_i, proj_j, pair_energies, tiles, rows, width
    )
    return updated, orbital_sums


def solution(mesh):
    split = Mesh(mesh.devices.reshape(4, 4, 4, 2), DEV)
    in_specs = (
        P(DEV, None, None),
        P(),
        P(DEV, None),
        P(DEV, None, None),
        P(DEV, None, None),
        P(DEV),
        P(DEV, None),
        P(),
    )
    out_specs = (P(DEV, None, None), P(DEV, None, None))
    return jax.shard_map(body, mesh=split, in_specs=in_specs, out_specs=out_specs, check_vma=False)
```
